512 devices in a mesh: band: 8 (over x, core), domain: 64 (over y, z).
Axes of the slice: x: 4, y: 8, z: 8, core: 2. Of those that a mesh axis runs over, the one named last changes fastest.
Arguments:
- dens_part: float32 [8, 171, 147456], P('band', None, 'domain'), may hold values from -3 to 3
- counts: int32 [64], P('domain'), may hold values from 1 to 2304, 49152 in all
- gaunt: float32 [171, 525], replicated, may hold values from -0.4375 to 0.4375
- pair_waves: float32 [21, 400], replicated, may hold values from -1.25 to 1.25
- y_table: float32 [25, 50], replicated, may hold values from -1.25 to 1.25
- core: float32 [400], replicated, may hold values from 1 to 4
- radial_weights: float32 [400], replicated, may hold values from 0.0001 to 0.001
Outputs:
- dh_packed: float32 [171, 147456], P(None, 'domain')
- atom_energy: float32 [147456], P('domain')
The draws below stay inside these ranges and needn't reach their ends.
Inputs may be any that keep to these rules, and one draw needn't show every extreme that they name: `counts`: atoms owned by each domain; they sum to 49152, and some domain owns exactly 2304.
All inputs are finite; a program needn't handle non-finite values. No bound on the sum of `counts` on one device may be relied on, other than what follows from the above.
Results may differ from the reference program's by a relative error of at most 0.0003.
Values sent between devices are 32-bit elements; how exact they have to be, the bound alone decides.
No kernel may reach another device: no remote copies, remote signals or barrier semaphores. Data moves between devices by JAX's collectives and lax.ppermute only.
A program may use at most 128 MiB of HBM per device.

```python
import math
import jax
import jax.numpy as jnp
import numpy as np
from jax import lax

NP = 171
NQ = 21
LM = 25
NDIR = 50
G = 400
ATOM_DEV = 768
SLOTS = 2304
N_BAND = 8
N_DOMAIN = 64


def block_levels(own_key, shape, shards, smallest, high):
    level = 1.0
    for position, parts in shards:
        steps = jax.random.uniform(jax.random.fold_in(jax.random.fold_in(own_key, 6), position), (parts,), jnp.float32, smallest / len(shards), high / len(shards))
        level = level * jnp.repeat(jnp.exp(steps), shape[position] // parts).reshape((-1,) + (1,) * (len(shape) - 1 - position))
    return level


def profile(amount, total, bound, skew):
    portions = [(1 << 20) // math.isqrt(grade ** skew) + 1 for grade in range(2, amount + 1)]
    rest, given = total - bound - (amount - 1), [1] * (amount - 1)
    while rest > 0:
        movable = [i for i in range(amount - 1) if given[i] < bound]
        pool, left = sum([portions[i] for i in movable]), rest
        for i in movable:
            more = min(bound - given[i], max(1, left * portions[i] // pool), rest)
            given[i] = given[i] + more
            rest = rest - more
    return np.array([bound] + given)


def ragged_sizes(own_key, count, total, limit, lean):
    if count == 2:
        one = jax.random.randint(own_key, (), max(1, total - limit), min(limit, total - 1) + 1)
        return jnp.stack([one, total - one])
    tallies = jnp.asarray(profile(count, total, limit, lean), jnp.int32)
    couples = (count - 1) // 2
    source_of, taker = tallies[1:1 + 2 * couples:2], tallies[2:2 + 2 * couples:2]
    room = jnp.minimum(source_of - 1, limit - taker)
    passed = jax.random.randint(jax.random.fold_in(own_key, 1), (couples,), 0, 1 << 20) % (room + 1)
    tallies = tallies.at[1:1 + 2 * couples:2].set(source_of - passed).at[2:2 + 2 * couples:2].set(taker + passed)
    return tallies[jax.random.permutation(jax.random.fold_in(own_key, 2), count)]


def bell_draw(rng, shape, scale, limit, split=(), held_as=jnp.bfloat16):
    array = scale * jax.random.normal(rng, shape, jnp.float32)
    if split:
        array = array * block_levels(rng, shape, split, -0.22, 0.18)
    return jnp.clip(array, -limit, limit).astype(held_as)


def setup_inputs(seed: int = 0) -> dict:
    streams_of = jax.random.split(jax.random.key(seed), 8)
    dens_part = bell_draw(streams_of[0], (N_BAND, NP, N_DOMAIN * SLOTS), 0.35, 3.0, ((0, 8), (2, 64)), jnp.float32)
    counts = ragged_sizes(streams_of[1], N_DOMAIN, ATOM_DEV * N_DOMAIN, SLOTS, 2).astype(jnp.int32)
    gaunt = bell_draw(streams_of[2], (NP, LM * NQ), NP ** -0.5, 0.4375, (), jnp.float32)
    pair_waves = bell_draw(streams_of[3], (NQ, G), NQ ** -0.5, 1.25, (), jnp.float32)
    y_table = bell_draw(streams_of[4], (LM, NDIR), LM ** -0.5, 1.25, (), jnp.float32)
    core = jnp.clip(jnp.exp(jax.random.uniform(streams_of[5], (G,), jnp.float32, math.log(1.0), math.log(4.0))), 1.0, 4.0)
    radial_weights = jnp.clip(jnp.exp(jax.random.uniform(streams_of[6], (G,), jnp.float32, math.log(0.0001), math.log(0.001))), 0.0001, 0.001)
    return {"dens_part": dens_part, "counts": counts, "gaunt": gaunt, "pair_waves": pair_waves, "y_table": y_table, "core": core, "radial_weights": radial_weights}


highest = lax.Precision.HIGHEST

def local_energy(density_rows, gaunt, pair_waves, y_table, core, radial_weights):
    atom_count = density_rows.shape[0]
    harmonics = y_table.shape[0]
    pair_count = pair_waves.shape[0]
    directions = y_table.shape[1]
    coefficients = jnp.dot(density_rows, gaunt, precision=highest, preferred_element_type=jnp.float32)
    coefficients = coefficients.reshape(atom_count * harmonics, pair_count)
    radial = jnp.dot(coefficients, pair_waves, precision=highest, preferred_element_type=jnp.float32)
    radial = radial.reshape(atom_count, harmonics, pair_waves.shape[1])
    points = jnp.einsum('ln,alg->ang', y_table, radial, precision=highest) + core[None, None, :]
    smooth = jnp.sqrt(points * points + 0.25)
    cube_root = jnp.cbrt(smooth)
    wigner_radius = 0.6203504908994 / cube_root
    denominator = 7.8 + wigner_radius
    energy_density = -0.7385587663820224 * smooth * cube_root - 0.44 * smooth / denominator
    slope = -0.9847450218426965 * cube_root - 0.44 * (1.0 / denominator + wigner_radius / (3.0 * denominator * denominator))
    point_weight = 4.0 * jnp.pi / directions * radial_weights
    energy = lax.optimization_barrier(jnp.sum(energy_density * point_weight[None, None, :], axis=(1, 2)))
    potential = point_weight[None, None, :] * slope * points / smooth
    back_radial = jnp.einsum('ln,ang->alg', y_table, potential, precision=highest)
    back_coef = jnp.dot(back_radial.reshape(atom_count * harmonics, pair_waves.shape[1]), pair_waves.T, precision=highest, preferred_element_type=jnp.float32)
    back_coef = back_coef.reshape(atom_count, harmonics * pair_count)
    hamiltonian = jnp.dot(back_coef, gaunt.T, precision=highest, preferred_element_type=jnp.float32)
    return (hamiltonian, energy)

def reference(dens_part, counts, gaunt, pair_waves, y_table, core, radial_weights):
    density = lax.optimization_barrier(jnp.sum(dens_part, axis=0)).T.reshape(N_DOMAIN, SLOTS, NP)
    slot_ids = jnp.arange(SLOTS).astype(jnp.int32)

    def per_domain(packed):
        block, owned = packed
        is_alive = slot_ids < owned
        block = jnp.where(is_alive[:, None], block, jnp.zeros_like(block))
        hamiltonian, energy = local_energy(block, gaunt, pair_waves, y_table, core, radial_weights)
        hamiltonian = jnp.where(is_alive[:, None], hamiltonian, jnp.zeros_like(hamiltonian))
        energy = jnp.where(is_alive, energy, jnp.zeros_like(energy))
        return (hamiltonian, energy)
    hamiltonian, energy = lax.map(per_domain, (density, counts.astype(jnp.int32)))
    return (hamiltonian.reshape(N_DOMAIN * SLOTS, NP).T, energy.reshape(N_DOMAIN * SLOTS))
```

```python
import functools

import jax
import jax.numpy as jnp
from jax import lax
from jax.experimental import pallas as pl
from jax.experimental.pallas import tpu as pltpu
from jax.sharding import PartitionSpec as P

highest = lax.Precision.HIGHEST
LANES = 128
QROWS = 32
PROWS = 192
GROUP = 14
RADIUS = 0.6203504908994
SLOPE = 0.44 * RADIUS / 3.0 / 7.8**2
SLOPE_SHIFT = 0.5 * (0.44 / 7.8) / SLOPE
SLOPE_REST = 0.9847450218426965 / SLOPE - SLOPE_SHIFT**2
ENERGY = 0.44 / 7.8
ENERGY_SHIFT = 0.7385587663820224 / ENERGY


def halves(x):
    high = x.astype(jnp.bfloat16)
    return high, (x - high.astype(jnp.float32)).astype(jnp.bfloat16)


def dot(a, b):
    return jnp.dot(a, b, preferred_element_type=jnp.float32)


def point_terms(points):
    log = jnp.log2(points * points + 0.25)
    t = jnp.exp2(log * (1.0 / 6.0))
    square = t * t
    share = 1.0 / (t + RADIUS / 7.8)
    energy = (square * square) * (share + ENERGY_SHIFT)
    shifted = share + SLOPE_SHIFT
    return energy, (points * (1.0 / square)) * (shifted * shifted + SLOPE_REST)


def evaluate_blocks(pairs, part_of, b_ref, c_ref, e_ref, lhs_p_ref, lhs_b_ref, p_refs, v_refs):
    grid_rows = lhs_p_ref.shape[0]
    cut = 208
    steps = [slice(0, 64), slice(64, 128), slice(128, 208), slice(208, 272), slice(272, 336), slice(336, 400)]

    def point_rhs(g):
        pieces = b_ref[pl.ds(2 * g, 2)]
        high, low = halves(jnp.concatenate([pieces[0], pieces[1]], axis=1))
        return jnp.concatenate([high, low, high], axis=0)

    def back(cols, high, low):
        first = dot(lhs_b_ref[:, cols], high)
        total = first[:QROWS] + first[QROWS:] + dot(lhs_b_ref[:QROWS, cols], low)
        return jnp.stack([total[:, :LANES], total[:, LANES:]])

    def finish(g, v_ref):
        c_ref[pl.ds(2 * g + 2, 2)] += back(slice(cut, grid_rows), v_ref[0, : grid_rows - cut, :], v_ref[1, : grid_rows - cut, :])

    def phase(g, now):
        other = 1 - now
        part = part_of(g)
        rhs = point_rhs(g + 1)
        finish(g - 1, v_refs[other])
        highs, lows = [], []
        for rows in steps:
            p_refs[other][rows, :] = dot(lhs_p_ref[rows, :], rhs)
            energy, potential = point_terms(p_refs[now][rows, :])
            e_ref[part, rows, :] += energy[:, :LANES] + energy[:, LANES:]
            high, low = halves(potential)
            if rows.stop <= cut:
                highs.append(high)
                lows.append(low)
                if rows.stop == cut:
                    c_ref[pl.ds(2 * g + 2, 2)] = back(
                        slice(0, cut), jnp.concatenate(highs, axis=0), jnp.concatenate(lows, axis=0)
                    )
            else:
                late = slice(rows.start - cut, rows.stop - cut)
                v_refs[now][0, late, :] = high
                v_refs[now][1, late, :] = low

    rhs = point_rhs(0)
    for rows in steps:
        p_refs[0][rows, :] = dot(lhs_p_ref[rows, :], rhs)

    def several(j, carry):
        for i in range(4):
            phase(4 * j + i, i % 2)
        return carry

    lax.fori_loop(0, pairs // 4, several, 0)
    for g in range(pairs // 4 * 4, pairs):
        phase(g, g % 2)
    finish(pairs - 1, v_refs[(pairs - 1) % 2])


def band_sum(recv_ref, rows):
    total = recv_ref[0, rows, :]
    for k in range(1, recv_ref.shape[0]):
        total = total + recv_ref[k, rows, :]
    return total


def row_pad(x, rows):
    return jnp.concatenate([x, jnp.zeros((rows - x.shape[0], x.shape[1]), jnp.float32)], axis=0)


def masked_density(total, live):
    rows = lax.broadcasted_iota(jnp.int32, total.shape, 0)
    density = jnp.where(live & (rows < 171), total, 0.0)
    return jnp.where((rows == 171) | (rows == 172), 1.0, density)


def energy_line(e_ref, part, weight_ref):
    return jnp.sum(e_ref[part] * weight_ref[...], axis=0, keepdims=True)


def forward(table, high, low):
    return dot(table, jnp.concatenate([high, high], axis=0)) + dot(table[:, :PROWS], low)


def wide_start(recv_ref, at, live, mt, mt_copy, b_ref, directions):
    total = row_pad(band_sum(recv_ref, slice(at, recv_ref.shape[1])), PROWS)
    dh, dl = halves(masked_density(total, live))
    mt_copy.wait()
    blocks = forward(mt[: directions * QROWS, :], dh, dl)
    b_ref[:directions] = blocks.reshape(directions, QROWS, LANES)


def wide_finish(c_ref, m_hl, live, directions):
    ch, cl = halves(c_ref[2 : 2 + directions].reshape(directions * QROWS, LANES))
    first = dot(m_hl[:, : directions * QROWS], ch)
    ham = first[:PROWS] + first[PROWS:] + dot(m_hl[:PROWS, : directions * QROWS], cl)
    return jnp.where(live, ham, 0.0)[:171]


def narrow_start(recv_ref, live, mt, b_ref, at):
    total = band_sum(recv_ref, slice(0, 48))
    pieces = [total[:, 32 * i : 32 * i + 32] for i in range(4)]
    spread = jnp.concatenate([jnp.concatenate([p] * 4, axis=1) for p in pieces], axis=0)
    density = masked_density(spread, live)
    lane_group = lax.broadcasted_iota(jnp.int32, density.shape, 1) // 32
    blocks = jnp.zeros((GROUP * QROWS, LANES), jnp.float32)
    for i in range(4):
        high, low = halves(jnp.where(lane_group == i, density, 0.0))
        rows = slice(i * GROUP * QROWS, (i + 1) * GROUP * QROWS)
        blocks = blocks + forward(mt[rows, :], high, low)
    b_ref[at : at + GROUP] = blocks.reshape(GROUP, QROWS, LANES)


def narrow_finish(c_ref, m_hl, line, live, at):
    ch, cl = halves(c_ref[at + 2 : at + 2 + GROUP].reshape(GROUP * QROWS, LANES))
    lanes = lax.broadcasted_iota(jnp.int32, (PROWS, LANES), 1) // 32
    ham = jnp.zeros((PROWS, LANES), jnp.float32)
    for i in range(4):
        cols = slice(i * GROUP * QROWS, (i + 1) * GROUP * QROWS)
        table = m_hl[:, cols]
        first = dot(table, ch)
        part = first[:PROWS] + first[PROWS:] + dot(table[:PROWS], cl)
        ham = ham + jnp.where(lanes == i, part, 0.0)
    rows = lax.broadcasted_iota(jnp.int32, (PROWS, LANES), 0)
    ham = jnp.where(rows == 171, line, ham)
    ham = sum(ham[:, 32 * i : 32 * i + 32] for i in range(4))
    packed = jnp.concatenate([ham[48 * i : 48 * i + 48] for i in range(4)], axis=1)
    return jnp.where(live, packed, 0.0)


def chunk_kernel(base, narrow_base, copies, directions, scal_ref, recv_ref, *refs):
    mt_far, m_far, lhs_p, lhs_b, weight = refs[:5]
    out_ref, b_ref, c_ref, e_ref, p0, p1, v0, v1, mt, m_hl, sem = refs[5:]
    mt_copy = pltpu.make_async_copy(mt_far, mt, sem.at[0])
    mt_copy.start()
    m_copy = pltpu.make_async_copy(m_far, m_hl, sem.at[1])
    m_copy.start()
    lane = lax.broadcasted_iota(jnp.int32, (1, LANES), 1)
    live = base + scal_ref[1] * LANES + lane < scal_ref[0]
    e_ref[...] = jnp.zeros_like(e_ref)
    wide_start(recv_ref, 0 if narrow_base is None else 48, live, mt, mt_copy, b_ref, directions)
    pairs, part_of = directions // 2, lambda g: 0
    if narrow_base is not None:
        narrow_live = narrow_base + scal_ref[1] * 32 + lane % 32 < scal_ref[0]
        narrow_start(recv_ref, narrow_live, mt, b_ref, directions)
        filled = pairs + (directions - 3 * GROUP) // 2
        part_of = lambda g, wide=pairs: (g >= wide).astype(jnp.int32) + (g >= filled).astype(jnp.int32) if not isinstance(g, int) else int(g >= wide) + int(g >= filled)
        pairs = pairs + GROUP // 2
    evaluate_blocks(pairs, part_of, b_ref, c_ref, e_ref, lhs_p, lhs_b, (p0, p1), (v0, v1))
    m_copy.wait()
    energy = jnp.where(live, energy_line(e_ref, 0, weight), 0.0)
    pieces = [jnp.broadcast_to(energy, (8, LANES))]
    if narrow_base is not None:
        line = energy_line(e_ref, 1, weight) + jnp.where(lane < 96, energy_line(e_ref, 2, weight), 0.0)
        pieces.append(narrow_finish(c_ref, m_hl, line, narrow_live, directions))
    pieces.append(wide_finish(c_ref, m_hl, live, directions))
    at = 0
    for piece in pieces:
        rows = slice(at, at + piece.shape[0])
        for k in range(copies):
            out_ref[k, rows, :] = piece
        at += piece.shape[0]


def chunk_call(base, narrow_base, copies, directions, scal, recv, tables):
    narrow = narrow_base is not None
    tables = [pltpu.with_memory_space_constraint(t, pltpu.HBM) for t in tables[:2]] + list(tables[2:])
    shape = (copies, 179 + 48 * narrow, LANES)
    blocks = directions + GROUP * narrow
    grid_rows = tables[2].shape[0]
    return pl.pallas_call(
        functools.partial(chunk_kernel, base, narrow_base, copies, directions),
        out_shape=jax.ShapeDtypeStruct(shape, jnp.float32),
        in_specs=[pl.BlockSpec(memory_space=pltpu.SMEM)]
        + [pl.BlockSpec(memory_space=pltpu.VMEM)]
        + [pl.BlockSpec(memory_space=pltpu.HBM)] * 2
        + [pl.BlockSpec(memory_space=pltpu.VMEM)] * 3,
        out_specs=pl.BlockSpec(memory_space=pltpu.VMEM),
        scratch_shapes=[pltpu.VMEM((blocks + 2, QROWS, LANES), jnp.float32)] * 2
        + [pltpu.VMEM((1 + 2 * narrow, grid_rows, LANES), jnp.float32)]
        + [pltpu.VMEM((grid_rows, 2 * LANES), jnp.float32)] * 2
        + [pltpu.VMEM((2, grid_rows, 2 * LANES), jnp.bfloat16)] * 2
        + [pltpu.VMEM(t.shape, jnp.bfloat16) for t in tables[:2]]
        + [pltpu.SemaphoreType.DMA((2,))],
        cost_estimate=pl.CostEstimate(flops=8_000_000_000, bytes_accessed=4_000_000, transcendentals=10_000_000),
        compiler_params=pltpu.CompilerParams(vmem_limit_bytes=18 * 1024 * 1024),
    )(scal, recv, *tables)


def table_kernel(gaunt_ref, waves_ref, y_ref, core_ref, rw_ref, mt_far, m_far, lhs_p, lhs_b, weight_ref, *scratch):
    gt_ref, mf_ref, mt_ref, m_hl, sem = scratch
    entries, columns = gaunt_ref.shape
    pairs, grid = waves_ref.shape
    harmonics, directions = y_ref.shape
    gt_pad = jnp.concatenate([gaunt_ref[...], jnp.zeros((256 - entries, columns), jnp.float32)], axis=0)
    gt_pad = jnp.concatenate([gt_pad, jnp.zeros((256, 640 - columns), jnp.float32)], axis=1)
    turned = gt_pad.T
    gt_ref[0] = turned[:, :LANES]
    gt_ref[1] = turned[:, LANES:]
    mf_ref[...] = jnp.zeros_like(mf_ref)
    for q in range(pairs):
        for half in range(2):
            part = gt_ref[half, pl.ds(q, harmonics, stride=pairs), :]
            made = lax.dot_general(
                y_ref[...], part, (((0,), (0,)), ((), ())), precision=highest, preferred_element_type=jnp.float32
            )
            mf_ref[half, pl.ds(q, directions, stride=QROWS), :] = made
    m = jnp.concatenate([mf_ref[0], mf_ref[1]], axis=1)
    mh, ml = halves(m.T[:PROWS])
    m_hl[:PROWS, :] = mh
    m_hl[PROWS:, :] = ml
    m_copy = pltpu.make_async_copy(m_hl, m_far, sem.at[0])
    m_copy.start()
    m = m[:, :PROWS]
    row = lax.broadcasted_iota(jnp.int32, m.shape, 0)
    col = lax.broadcasted_iota(jnp.int32, m.shape, 1)
    kind = row % QROWS
    unit = (row < directions * QROWS) & (((kind == 21) & (col == 171)) | ((kind == 22) & (col == 172)))
    high, low = halves(jnp.where(unit, 1.0, m))
    mt_ref[...] = jnp.concatenate([high, low], axis=1)
    mt_copy = pltpu.make_async_copy(mt_ref, mt_far, sem.at[1])
    mt_copy.start()
    waves = waves_ref[...]
    back = lambda x: x.astype(jnp.float32)
    wh = back(waves.astype(jnp.bfloat16))
    wl = waves - wh
    core = core_ref[...]
    ch = back(core.astype(jnp.bfloat16))
    cm = back((core - ch).astype(jnp.bfloat16))
    cl = core - ch - cm
    gap = lambda n: jnp.zeros((n, grid), jnp.float32)
    stack = jnp.concatenate(
        [wh, ch, cl, gap(QROWS - pairs - 2), wh, gap(QROWS - pairs), wl, cm, gap(QROWS - pairs - 1), gap(32)], axis=0
    )
    stack = jnp.concatenate([stack, jnp.zeros((LANES, 512 - grid), jnp.float32)], axis=1)
    lhs_p[...] = stack.T[:grid, :96].astype(jnp.bfloat16)
    weight = -(4.0 * jnp.pi / directions) * rw_ref[...]
    bh, bl = halves(jnp.concatenate([waves * (SLOPE * weight), gap(QROWS - pairs)], axis=0))
    lhs_b[...] = jnp.concatenate([bh, bl], axis=0)
    wide = jnp.concatenate([jnp.broadcast_to(ENERGY * weight, (LANES, grid)), jnp.zeros((LANES, 512 - grid), jnp.float32)], axis=1)
    weight_ref[...] = wide.T[:grid]
    m_copy.wait()
    mt_copy.wait()


def make_tables(gaunt, pair_waves, y_table, core, radial_weights):
    grid = core.shape[0]
    rows = 4 * GROUP * QROWS
    return pl.pallas_call(
        table_kernel,
        out_shape=(
            pltpu.HBM((rows, 2 * PROWS), jnp.bfloat16),
            pltpu.HBM((2 * PROWS, rows), jnp.bfloat16),
            jax.ShapeDtypeStruct((grid, 96), jnp.bfloat16),
            jax.ShapeDtypeStruct((2 * QROWS, grid), jnp.bfloat16),
            jax.ShapeDtypeStruct((grid, LANES), jnp.float32),
        ),
        in_specs=[pl.BlockSpec(memory_space=pltpu.VMEM)] * 5,
        out_specs=[pl.BlockSpec(memory_space=pltpu.HBM)] * 2 + [pl.BlockSpec(memory_space=pltpu.VMEM)] * 3,
        scratch_shapes=[
            pltpu.VMEM((2, 640, LANES), jnp.float32),
            pltpu.VMEM((2, rows, LANES), jnp.float32),
            pltpu.VMEM((rows, 2 * PROWS), jnp.bfloat16),
            pltpu.VMEM((2 * PROWS, rows), jnp.bfloat16),
            pltpu.SemaphoreType.DMA((2,)),
        ],
        cost_estimate=pl.CostEstimate(flops=2_000_000_000, bytes_accessed=4_000_000, transcendentals=0),
        compiler_params=pltpu.CompilerParams(vmem_limit_bytes=18 * 1024 * 1024),
    )(gaunt, pair_waves, y_table, core.reshape(1, grid), radial_weights.reshape(1, grid))


def send_a_kernel(block_ref, out_ref, sem):
    copies = [
        pltpu.make_async_copy(block_ref.at[:, 0, pl.ds(LANES * k, LANES)], out_ref.at[k], sem.at[k]) for k in range(8)
    ]
    for copy in copies:
        copy.start()
    for copy in copies:
        copy.wait()


def send_b_kernel(block_ref, out_ref, tail_ref, sem):
    entries = block_ref.shape[0]
    tail = pltpu.make_async_copy(block_ref.at[:, 0, pl.ds(2048, 256)], tail_ref, sem.at[8])
    tail.start()
    copies = [
        pltpu.make_async_copy(
            block_ref.at[:, 0, pl.ds(1024 + LANES * k, LANES)], out_ref.at[k, pl.ds(48, entries)], sem.at[k]
        )
        for k in range(8)
    ]
    for copy in copies:
        copy.start()
    tail.wait()
    rows = row_pad(tail_ref[...], PROWS)
    for k in range(8):
        own = rows[:, 32 * k : 32 * k + 32]
        out_ref[k, :48, :] = jnp.concatenate([own[48 * i : 48 * i + 48] for i in range(4)], axis=1)
    for copy in copies:
        copy.wait()


def send_call(kernel, rows, scratch, block):
    return pl.pallas_call(
        kernel,
        out_shape=jax.ShapeDtypeStruct((8, rows, LANES), jnp.float32),
        in_specs=[pl.BlockSpec(memory_space=pltpu.HBM)],
        out_specs=pl.BlockSpec(memory_space=pltpu.VMEM),
        scratch_shapes=scratch,
        cost_estimate=pl.CostEstimate(flops=100_000_000, bytes_accessed=1_500_000, transcendentals=0),
        compiler_params=pltpu.CompilerParams(vmem_limit_bytes=67_000_000),
    )(block)


def assemble_kernel(a_ref, b_ref, ham_ref, energy_ref, tail_ref, sem):
    copies = []
    for k in range(8):
        for part, ref, at in ((0, a_ref, 8), (1, b_ref, 56)):
            target = ham_ref.at[:, pl.ds(1024 * part + LANES * k, LANES)]
            copies.append(pltpu.make_async_copy(ref.at[k, pl.ds(at, 171)], target, sem.at[8 * part + k]))
    for copy in copies:
        copy.start()
    for i in range(4):
        rows = jnp.concatenate([b_ref[k, 8:56, 32 * i : 32 * i + 32] for k in range(8)], axis=1)
        if i < 3:
            tail_ref[48 * i : 48 * i + 48, :] = rows
        else:
            tail_ref[144:171, :] = rows[:27]
            energy_ref[16:18, :] = jnp.concatenate([rows[27:28, :LANES], rows[27:28, LANES:]], axis=0)
    tail = pltpu.make_async_copy(tail_ref, ham_ref.at[:, pl.ds(2048, 256)], sem.at[16])
    tail.start()
    for k in range(8):
        energy_ref[k : k + 1, :] = a_ref[k, 0:1, :]
        energy_ref[8 + k : 9 + k, :] = b_ref[k, 0:1, :]
    for copy in copies:
        copy.wait()
    tail.wait()


def assemble(all_a, all_b):
    return pl.pallas_call(
        assemble_kernel,
        out_shape=(jax.ShapeDtypeStruct((171, 2304), jnp.float32), jax.ShapeDtypeStruct((18, LANES), jnp.float32)),
        in_specs=[pl.BlockSpec(memory_space=pltpu.VMEM)] * 2,
        out_specs=[pl.BlockSpec(memory_space=pltpu.HBM), pl.BlockSpec(memory_space=pltpu.VMEM)],
        scratch_shapes=[pltpu.VMEM((171, 256), jnp.float32), pltpu.SemaphoreType.DMA((17,))],
        cost_estimate=pl.CostEstimate(flops=100_000_000, bytes_accessed=3_000_000, transcendentals=0),
        compiler_params=pltpu.CompilerParams(vmem_limit_bytes=8 * 1024 * 1024),
    )(all_a, all_b)


def per_device(dens_part, counts, gaunt, pair_waves, y_table, core, radial_weights):
    band_index = lax.axis_index("band").astype(jnp.int32)
    scal = jnp.stack([counts[0].astype(jnp.int32), band_index])
    directions = y_table.shape[1]
    rows = dens_part.transpose(1, 0, 2)
    send_a = send_call(send_a_kernel, 171, [pltpu.SemaphoreType.DMA((8,))], rows)
    recv_a = lax.all_to_all(send_a, "band", 0, 0, tiled=True)
    send_b = send_call(
        send_b_kernel, 219, [pltpu.VMEM((171, 256), jnp.float32), pltpu.SemaphoreType.DMA((9,))], rows
    )
    recv_b = lax.all_to_all(send_b, "band", 0, 0, tiled=True)
    tables = make_tables(gaunt, pair_waves, y_table, core, radial_weights)
    out_a = chunk_call(0, None, 8, directions, scal, recv_a, tables)
    all_a = lax.all_to_all(out_a, "band", 0, 0, tiled=True)
    out_b = chunk_call(1024, 2048, 1, directions, scal, recv_b, tables)
    all_b = lax.all_gather(out_b[0], "band", axis=0)
    ham, energy = assemble(all_a, all_b)
    return ham, energy.reshape(18 * LANES)


def solution(mesh):
    return jax.shard_map(
        per_device,
        mesh=mesh,
        in_specs=(P("band", None, "domain"), P("domain"), P(), P(), P(), P(), P()),
        out_specs=(P(None, "domain"), P("domain")),
        check_vma=False,
    )
```

```python
import functools

import jax
import jax.numpy as jnp
from jax import lax
from jax.experimental import pallas as pl
from jax.experimental.pallas import tpu as pltpu
from jax.sharding import PartitionSpec as P

highest = lax.Precision.HIGHEST
LANES = 128
QROWS = 32
PROWS = 192
GROUP = 14
RADIUS = 0.6203504908994
SLOPE = 0.44 * RADIUS / 3.0 / 7.8**2
SLOPE_SHIFT = 0.5 * (0.44 / 7.8) / SLOPE
SLOPE_REST = 0.9847450218426965 / SLOPE - SLOPE_SHIFT**2
ENERGY = 0.44 / 7.8
ENERGY_SHIFT = 0.7385587663820224 / ENERGY


def halves(x):
    high = x.astype(jnp.bfloat16)
    return high, (x - high.astype(jnp.float32)).astype(jnp.bfloat16)


def dot(a, b):
    return jnp.dot(a, b, preferred_element_type=jnp.float32)


def point_terms(points):
    log = jnp.log2(points * points + 0.25)
    t = jnp.exp2(log * (1.0 / 6.0))
    square = t * t
    share = 1.0 / (t + RADIUS / 7.8)
    energy = (square * square) * (share + ENERGY_SHIFT)
    shifted = share + SLOPE_SHIFT
    return energy, (points * (1.0 / square)) * (shifted * shifted + SLOPE_REST)


def evaluate_blocks(pairs, part_of, b_ref, c_ref, e_ref, lhs_p_ref, lhs_b_ref, p_refs, v_refs):
    grid_rows = lhs_p_ref.shape[0]
    cut = 208
    steps = [slice(0, 64), slice(64, 128), slice(128, 208), slice(208, 272), slice(272, 336), slice(336, 400)]

    def point_rhs(g):
        pieces = b_ref[pl.ds(2 * g, 2)]
        high, low = halves(jnp.concatenate([pieces[0], pieces[1]], axis=1))
        return jnp.concatenate([high, low, high], axis=0)

    def back(cols, high, low):
        first = dot(lhs_b_ref[:, cols], high)
        total = first[:QROWS] + first[QROWS:] + dot(lhs_b_ref[:QROWS, cols], low)
        return jnp.stack([total[:, :LANES], total[:, LANES:]])

    def finish(g, v_ref):
        c_ref[pl.ds(2 * g + 2, 2)] += back(slice(cut, grid_rows), v_ref[0, : grid_rows - cut, :], v_ref[1, : grid_rows - cut, :])

    def phase(g, now):
        other = 1 - now
        part = part_of(g)
        rhs = point_rhs(g + 1)
        finish(g - 1, v_refs[other])
        highs, lows = [], []
        for rows in steps:
            p_refs[other][rows, :] = dot(lhs_p_ref[rows, :], rhs)
            energy, potential = point_terms(p_refs[now][rows, :])
            e_ref[part, rows, :] += energy[:, :LANES] + energy[:, LANES:]
            high, low = halves(potential)
            if rows.stop <= cut:
                highs.append(high)
                lows.append(low)
                if rows.stop == cut:
                    c_ref[pl.ds(2 * g + 2, 2)] = back(
                        slice(0, cut), jnp.concatenate(highs, axis=0), jnp.concatenate(lows, axis=0)
                    )
            else:
                late = slice(rows.start - cut, rows.stop - cut)
                v_refs[now][0, late, :] = high
                v_refs[now][1, late, :] = low

    rhs = point_rhs(0)
    for rows in steps:
        p_refs[0][rows, :] = dot(lhs_p_ref[rows, :], rhs)

    def several(j, carry):
        for i in range(4):
            phase(4 * j + i, i % 2)
        return carry

    lax.fori_loop(0, pairs // 4, several, 0)
    for g in range(pairs // 4 * 4, pairs):
        phase(g, g % 2)
    finish(pairs - 1, v_refs[(pairs - 1) % 2])


def band_sum(recv_ref, rows):
    total = recv_ref[0, rows, :]
    for k in range(1, recv_ref.shape[0]):
        total = total + recv_ref[k, rows, :]
    return total


def row_pad(x, rows):
    return jnp.concatenate([x, jnp.zeros((rows - x.shape[0], x.shape[1]), jnp.float32)], axis=0)


def masked_density(total, live):
    rows = lax.broadcasted_iota(jnp.int32, total.shape, 0)
    density = jnp.where(live & (rows < 171), total, 0.0)
    return jnp.where((rows == 171) | (rows == 172), 1.0, density)


def energy_line(e_ref, part, weight_ref):
    return jnp.sum(e_ref[part] * weight_ref[...], axis=0, keepdims=True)


def forward(table, high, low):
    return dot(table, jnp.concatenate([high, high], axis=0)) + dot(table[:, :PROWS], low)


def start_blocks(recv_ref, lives, mt, b_ref, directions):
    lead = 48 * (len(lives) - 1)
    density = masked_density(row_pad(band_sum(recv_ref, slice(lead, recv_ref.shape[1])), PROWS), lives[0])
    if lead:
        total = band_sum(recv_ref, slice(0, lead))
        pieces = [total[:, 32 * i : 32 * i + 32] for i in range(4)]
        spread = jnp.concatenate([jnp.concatenate([p] * 4, axis=1) for p in pieces], axis=0)
        density = jnp.concatenate([density, masked_density(spread, lives[1])], axis=1)
    rows = directions * QROWS
    table = mt[...] if lead else mt[:rows, :]
    blocks = forward(table, *halves(density))
    b_ref[:directions] = blocks[:rows, :LANES].reshape(directions, QROWS, LANES)
    if lead:
        parts = blocks[:, LANES:].reshape(4, GROUP * QROWS, LANES)
        lane_group = lax.broadcasted_iota(jnp.int32, parts.shape[1:], 1) // 32
        chosen = parts[3]
        for i in range(3):
            chosen = jnp.where(lane_group == i, parts[i], chosen)
        b_ref[directions : directions + GROUP] = chosen.reshape(GROUP, QROWS, LANES)


def finish_blocks(c_ref, m_hl, lives, line, directions):
    rows = directions * QROWS
    sums = c_ref[2 : 2 + directions].reshape(rows, LANES)
    table = m_hl[:, :rows]
    if len(lives) > 1:
        table = m_hl[...]
        narrow = c_ref[directions + 2 : directions + 2 + GROUP].reshape(GROUP * QROWS, LANES)
        lane_group = lax.broadcasted_iota(jnp.int32, narrow.shape, 1) // 32
        spread = jnp.concatenate([jnp.where(lane_group == i, narrow, 0.0) for i in range(4)], axis=0)
        sums = jnp.concatenate([row_pad(sums, table.shape[1]), spread], axis=1)
    high, low = halves(sums)
    first = dot(table, high)
    ham = first[:PROWS] + first[PROWS:] + dot(table[:PROWS], low)
    wide = jnp.where(lives[0], ham[:171, :LANES], 0.0)
    if len(lives) == 1:
        return [wide]
    ham = ham[:, LANES:]
    kind = lax.broadcasted_iota(jnp.int32, (PROWS, LANES), 0)
    ham = jnp.where(kind == 171, line, ham)
    ham = sum(ham[:, 32 * i : 32 * i + 32] for i in range(4))
    packed = jnp.concatenate([ham[48 * i : 48 * i + 48] for i in range(4)], axis=1)
    return [jnp.where(lives[1], packed, 0.0), wide]


def chunk_kernel(base, narrow_base, copies, directions, owned_ref, recv_ref, *refs):
    mt, m_far, lhs_p, lhs_b, weight = refs[:5]
    out_ref, b_ref, c_ref, e_ref, p0, p1, v0, v1, m_hl, near_ref, sem = refs[5:]
    m_copy = pltpu.make_async_copy(m_far, m_hl, sem.at[copies])
    m_copy.start()
    lane = lax.broadcasted_iota(jnp.int32, (1, LANES), 1)
    lives = [base + lane < owned_ref[0:1, :]]
    pairs, part_of = directions // 2, lambda g: 0
    if narrow_base is not None:
        lives.append(narrow_base + lane % 32 < owned_ref[1:2, :])
        wide, filled = pairs, pairs + (directions - 3 * GROUP) // 2
        part_of = lambda g: jnp.where(g >= wide, 1, 0) + jnp.where(g >= filled, 1, 0)
        pairs = pairs + GROUP // 2
    e_ref[...] = jnp.zeros_like(e_ref)
    start_blocks(recv_ref, lives, mt, b_ref, directions)
    evaluate_blocks(pairs, part_of, b_ref, c_ref, e_ref, lhs_p, lhs_b, (p0, p1), (v0, v1))
    energy = jnp.where(lives[0], energy_line(e_ref, 0, weight), 0.0)
    line = None
    if narrow_base is not None:
        line = energy_line(e_ref, 1, weight) + jnp.where(lane < 96, energy_line(e_ref, 2, weight), 0.0)
    m_copy.wait()
    target = near_ref if copies > 1 else out_ref.at[0]
    at = 0
    for piece in [jnp.broadcast_to(energy, (8, LANES))] + finish_blocks(c_ref, m_hl, lives, line, directions):
        target[at : at + piece.shape[0], :] = piece
        at += piece.shape[0]
    if copies > 1:
        leaving = [pltpu.make_async_copy(near_ref, out_ref.at[k], sem.at[k]) for k in range(copies)]
        for copy in leaving:
            copy.start()
        for copy in leaving:
            copy.wait()


def chunk_call(base, narrow_base, copies, directions, owned, recv, tables):
    narrow = narrow_base is not None
    tables = [tables[0], pltpu.with_memory_space_constraint(tables[1], pltpu.HBM)] + list(tables[2:])
    shape = (copies, 179 + 48 * narrow, LANES)
    blocks = directions + GROUP * narrow
    grid_rows = tables[2].shape[0]
    return pl.pallas_call(
        functools.partial(chunk_kernel, base, narrow_base, copies, directions),
        out_shape=(pltpu.VMEM if copies == 1 else pltpu.HBM)(shape, jnp.float32),
        in_specs=[pl.BlockSpec(memory_space=pltpu.VMEM)] * 3
        + [pl.BlockSpec(memory_space=pltpu.HBM)]
        + [pl.BlockSpec(memory_space=pltpu.VMEM)] * 3,
        out_specs=pl.BlockSpec(memory_space=pltpu.VMEM if copies == 1 else pltpu.HBM),
        scratch_shapes=[pltpu.VMEM((blocks + 2, QROWS, LANES), jnp.float32)] * 2
        + [pltpu.VMEM((1 + 2 * narrow, grid_rows, LANES), jnp.float32)]
        + [pltpu.VMEM((grid_rows, 2 * LANES), jnp.float32)] * 2
        + [pltpu.VMEM((2, grid_rows, 2 * LANES), jnp.bfloat16)] * 2
        + [pltpu.VMEM(tables[1].shape, jnp.bfloat16)]
        + [pltpu.VMEM(shape[1:], jnp.float32), pltpu.SemaphoreType.DMA((copies + 1,))],
        cost_estimate=pl.CostEstimate(flops=8_000_000_000, bytes_accessed=4_000_000, transcendentals=10_000_000),
        compiler_params=pltpu.CompilerParams(vmem_limit_bytes=18 * 1024 * 1024),
    )(owned, recv, *tables)


def table_kernel(gaunt_ref, waves_ref, y_ref, core_ref, rw_ref, mt_ref, m_far, lhs_p, lhs_b, weight_ref, *scratch):
    gt_ref, mf_ref, m_hl, sem = scratch
    entries, columns = gaunt_ref.shape
    pairs, grid = waves_ref.shape
    harmonics, directions = y_ref.shape
    gt_pad = jnp.concatenate([gaunt_ref[...], jnp.zeros((256 - entries, columns), jnp.float32)], axis=0)
    gt_pad = jnp.concatenate([gt_pad, jnp.zeros((256, 640 - columns), jnp.float32)], axis=1)
    turned = gt_pad.T
    gt_ref[0] = turned[:, :LANES]
    gt_ref[1] = turned[:, LANES:]
    mf_ref[...] = jnp.zeros_like(mf_ref)
    for q in range(pairs):
        for half in range(2):
            part = gt_ref[half, pl.ds(q, harmonics, stride=pairs), :]
            made = lax.dot_general(
                y_ref[...], part, (((0,), (0,)), ((), ())), precision=highest, preferred_element_type=jnp.float32
            )
            mf_ref[half, pl.ds(q, directions, stride=QROWS), :] = made
    m = jnp.concatenate([mf_ref[0], mf_ref[1]], axis=1)
    mh, ml = halves(m.T[:PROWS])
    m_hl[:PROWS, :] = mh
    m_hl[PROWS:, :] = ml
    m_copy = pltpu.make_async_copy(m_hl, m_far, sem.at[0])
    m_copy.start()
    m = m[:, :PROWS]
    row = lax.broadcasted_iota(jnp.int32, m.shape, 0)
    col = lax.broadcasted_iota(jnp.int32, m.shape, 1)
    kind = row % QROWS
    unit = (row < directions * QROWS) & (((kind == 21) & (col == 171)) | ((kind == 22) & (col == 172)))
    high, low = halves(jnp.where(unit, 1.0, m))
    mt_ref[...] = jnp.concatenate([high, low], axis=1)
    waves = waves_ref[...]
    back = lambda x: x.astype(jnp.float32)
    wh = back(waves.astype(jnp.bfloat16))
    wl = waves - wh
    core = core_ref[...]
    ch = back(core.astype(jnp.bfloat16))
    cm = back((core - ch).astype(jnp.bfloat16))
    cl = core - ch - cm
    gap = lambda n: jnp.zeros((n, grid), jnp.float32)
    stack = jnp.concatenate(
        [wh, ch, cl, gap(QROWS - pairs - 2), wh, gap(QROWS - pairs), wl, cm, gap(QROWS - pairs - 1), gap(32)], axis=0
    )
    stack = jnp.concatenate([stack, jnp.zeros((LANES, 512 - grid), jnp.float32)], axis=1)
    lhs_p[...] = stack.T[:grid, :96].astype(jnp.bfloat16)
    weight = -(4.0 * jnp.pi / directions) * rw_ref[...]
    bh, bl = halves(jnp.concatenate([waves * (SLOPE * weight), gap(QROWS - pairs)], axis=0))
    lhs_b[...] = jnp.concatenate([bh, bl], axis=0)
    wide = jnp.concatenate([jnp.broadcast_to(ENERGY * weight, (LANES, grid)), jnp.zeros((LANES, 512 - grid), jnp.float32)], axis=1)
    weight_ref[...] = wide.T[:grid]
    m_copy.wait()


def make_tables(gaunt, pair_waves, y_table, core, radial_weights):
    grid = core.shape[0]
    rows = 4 * GROUP * QROWS
    return pl.pallas_call(
        table_kernel,
        out_shape=(
            jax.ShapeDtypeStruct((rows, 2 * PROWS), jnp.bfloat16),
            pltpu.HBM((2 * PROWS, rows), jnp.bfloat16),
            jax.ShapeDtypeStruct((grid, 96), jnp.bfloat16),
            jax.ShapeDtypeStruct((2 * QROWS, grid), jnp.bfloat16),
            jax.ShapeDtypeStruct((grid, LANES), jnp.float32),
        ),
        in_specs=[pl.BlockSpec(memory_space=pltpu.VMEM)] * 5,
        out_specs=[pl.BlockSpec(memory_space=pltpu.VMEM), pl.BlockSpec(memory_space=pltpu.HBM)]
        + [pl.BlockSpec(memory_space=pltpu.VMEM)] * 3,
        scratch_shapes=[
            pltpu.VMEM((2, 640, LANES), jnp.float32),
            pltpu.VMEM((2, rows, LANES), jnp.float32),
            pltpu.VMEM((2 * PROWS, rows), jnp.bfloat16),
            pltpu.SemaphoreType.DMA((1,)),
        ],
        cost_estimate=pl.CostEstimate(flops=2_000_000_000, bytes_accessed=4_000_000, transcendentals=0),
        compiler_params=pltpu.CompilerParams(vmem_limit_bytes=18 * 1024 * 1024),
    )(gaunt, pair_waves, y_table, core.reshape(1, grid), radial_weights.reshape(1, grid))


def send_kernel(first, narrow, block_ref, out_ref, near_ref, *scratch):
    entries = block_ref.shape[0]
    tail_ref, pack_ref, sem = scratch if narrow is not None else (None, None, *scratch)
    lead = 48 if narrow is not None else 0
    arrivals = [
        pltpu.make_async_copy(block_ref.at[:, 0, pl.ds(first + LANES * k, LANES)], near_ref.at[k], sem.at[k])
        for k in range(8)
    ]
    if narrow is not None:
        tail = pltpu.make_async_copy(block_ref.at[:, 0, pl.ds(narrow, 256)], tail_ref, sem.at[16])
        tail.start()
    for copy in arrivals:
        copy.start()
    leaving = []
    if narrow is not None:
        tail.wait()
        rows = row_pad(tail_ref[...], PROWS)
        for k in range(8):
            own = rows[:, 32 * k : 32 * k + 32]
            pack_ref[k] = jnp.concatenate([own[48 * i : 48 * i + 48] for i in range(4)], axis=1)
        leaving.append(pltpu.make_async_copy(pack_ref, out_ref.at[:, pl.ds(0, 48)], sem.at[17]))
        leaving[0].start()
    for k in range(8):
        arrivals[k].wait()
        copy = pltpu.make_async_copy(near_ref.at[k], out_ref.at[k, pl.ds(lead, entries)], sem.at[8 + k])
        copy.start()
        leaving.append(copy)
    for copy in leaving:
        copy.wait()


def send_call(first, narrow, rows):
    entries = rows.shape[0]
    scratch = [pltpu.VMEM((8, entries, LANES), jnp.float32)]
    if narrow is not None:
        scratch += [pltpu.VMEM((entries, 256), jnp.float32), pltpu.VMEM((8, 48, LANES), jnp.float32)]
    return pl.pallas_call(
        functools.partial(send_kernel, first, narrow),
        out_shape=pltpu.HBM((8, entries + (48 if narrow is not None else 0), LANES), jnp.float32),
        in_specs=[pl.BlockSpec(memory_space=pltpu.HBM)],
        out_specs=pl.BlockSpec(memory_space=pltpu.HBM),
        scratch_shapes=scratch + [pltpu.SemaphoreType.DMA((18,))],
        cost_estimate=pl.CostEstimate(flops=100_000_000, bytes_accessed=1_500_000, transcendentals=0),
        compiler_params=pltpu.CompilerParams(vmem_limit_bytes=6 * 1024 * 1024),
    )(rows)


def assemble_kernel(a_ref, b_ref, ham_ref, energy_far, tail_ref, energy_ref, sem):
    copies = []
    for k in range(8):
        for part, ref, at in ((0, a_ref, 56), (1, b_ref, 8)):
            target = ham_ref.at[:, pl.ds(1024 * part + LANES * k, LANES)]
            copies.append(pltpu.make_async_copy(ref.at[k, pl.ds(at, 171)], target, sem.at[8 * part + k]))
    for copy in copies:
        copy.start()
    for i in range(4):
        rows = jnp.concatenate([a_ref[k, 8:56, 32 * i : 32 * i + 32] for k in range(8)], axis=1)
        if i < 3:
            tail_ref[48 * i : 48 * i + 48, :] = rows
        else:
            tail_ref[144:171, :] = rows[:27]
            energy_ref[16:18, :] = jnp.concatenate([rows[27:28, :LANES], rows[27:28, LANES:]], axis=0)
    tail = pltpu.make_async_copy(tail_ref, ham_ref.at[:, pl.ds(2048, 256)], sem.at[16])
    tail.start()
    for k in range(8):
        energy_ref[k : k + 1, :] = a_ref[k, 0:1, :]
        energy_ref[8 + k : 9 + k, :] = b_ref[k, 0:1, :]
    energies = pltpu.make_async_copy(energy_ref, energy_far, sem.at[17])
    energies.start()
    for copy in copies:
        copy.wait()
    tail.wait()
    energies.wait()


def assemble(all_a, all_b):
    return pl.pallas_call(
        assemble_kernel,
        out_shape=(pltpu.HBM((171, 2304), jnp.float32), pltpu.HBM((18, LANES), jnp.float32)),
        in_specs=[pl.BlockSpec(memory_space=pltpu.VMEM)] * 2,
        out_specs=[pl.BlockSpec(memory_space=pltpu.HBM)] * 2,
        scratch_shapes=[
            pltpu.VMEM((171, 256), jnp.float32),
            pltpu.VMEM((18, LANES), jnp.float32),
            pltpu.SemaphoreType.DMA((18,)),
        ],
        cost_estimate=pl.CostEstimate(flops=100_000_000, bytes_accessed=3_000_000, transcendentals=0),
        compiler_params=pltpu.CompilerParams(vmem_limit_bytes=8 * 1024 * 1024),
    )(all_a, all_b)


def per_device(dens_part, counts, gaunt, pair_waves, y_table, core, radial_weights):
    band_index = lax.axis_index("band").astype(jnp.int32)
    widths = jnp.where(lax.broadcasted_iota(jnp.int32, (2, LANES), 0) == 0, LANES, 32)
    owned = counts[0].astype(jnp.int32) - band_index * widths
    directions = y_table.shape[1]
    rows = pltpu.with_memory_space_constraint(dens_part.transpose(1, 0, 2), pltpu.HBM)
    send_a = send_call(0, 2048, rows)
    recv_a = lax.all_to_all(send_a, "band", 0, 0, tiled=True)
    send_b = send_call(1024, None, rows)
    recv_b = lax.all_to_all(send_b, "band", 0, 0, tiled=True)
    tables = make_tables(gaunt, pair_waves, y_table, core, radial_weights)
    out_a = chunk_call(0, 2048, 8, directions, owned, recv_a, tables)
    all_a = lax.all_to_all(out_a, "band", 0, 0, tiled=True)
    out_b = chunk_call(1024, None, 1, directions, owned, recv_b, tables)
    all_b = lax.all_gather(out_b[0], "band", axis=0)
    ham, energy = assemble(all_a, all_b)
    return ham, energy.reshape(18 * LANES)


def solution(mesh):
    return jax.shard_map(
        per_device,
        mesh=mesh,
        in_specs=(P("band", None, "domain"), P("domain"), P(), P(), P(), P(), P()),
        out_specs=(P(None, "domain"), P("domain")),
        check_vma=False,
    )
```

```python
import functools

import jax
import jax.numpy as jnp
from jax import lax
from jax.experimental import pallas as pl
from jax.experimental.pallas import tpu as pltpu
from jax.sharding import PartitionSpec as P

highest = lax.Precision.HIGHEST
LANES = 128
QROWS = 32
PROWS = 192
GROUP = 14
RADIUS = 0.6203504908994
SLOPE = 0.44 * RADIUS / 3.0 / 7.8**2
SLOPE_SHIFT = 0.5 * (0.44 / 7.8) / SLOPE
SLOPE_REST = 0.9847450218426965 / SLOPE - SLOPE_SHIFT**2
ENERGY = 0.44 / 7.8
ENERGY_SHIFT = 0.7385587663820224 / ENERGY


def halves(x):
    high = x.astype(jnp.bfloat16)
    return high, (x - high.astype(jnp.float32)).astype(jnp.bfloat16)


def dot(a, b):
    return jnp.dot(a, b, preferred_element_type=jnp.float32)


def point_terms(points):
    log = jnp.log2(points * points + 0.25)
    t = jnp.exp2(log * (1.0 / 6.0))
    square = t * t
    share = 1.0 / (t + RADIUS / 7.8)
    energy = (square * square) * (share + ENERGY_SHIFT)
    shifted = share + SLOPE_SHIFT
    return energy, (points * (1.0 / square)) * (shifted * shifted + SLOPE_REST)


def evaluate_blocks(pairs, unroll, part_of, b_ref, c_ref, e_ref, lhs_p_ref, lhs_b_ref, p_refs, v_refs):
    grid_rows = lhs_p_ref.shape[0]
    cut = 208
    steps = [slice(0, 64), slice(64, 128), slice(128, 208), slice(208, 272), slice(272, 336), slice(336, 400)]

    def point_rhs(g):
        pieces = b_ref[pl.ds(2 * g, 2)]
        high, low = halves(jnp.concatenate([pieces[0], pieces[1]], axis=1))
        return jnp.concatenate([high, low, high], axis=0)

    def back(cols, high, low):
        first = dot(lhs_b_ref[:, cols], high)
        total = first[:QROWS] + first[QROWS:] + dot(lhs_b_ref[:QROWS, cols], low)
        return jnp.stack([total[:, :LANES], total[:, LANES:]])

    def finish(g, v_ref):
        c_ref[pl.ds(2 * g + 2, 2)] += back(slice(cut, grid_rows), v_ref[0, : grid_rows - cut, :], v_ref[1, : grid_rows - cut, :])

    def phase(g, now):
        other = 1 - now
        part = part_of(g)
        rhs = point_rhs(g + 1)
        finish(g - 1, v_refs[other])
        highs, lows = [], []
        for rows in steps:
            p_refs[other][rows, :] = dot(lhs_p_ref[rows, :], rhs)
            energy, potential = point_terms(p_refs[now][rows, :])
            e_ref[part, rows, :] += energy[:, :LANES] + energy[:, LANES:]
            high, low = halves(potential)
            if rows.stop <= cut:
                highs.append(high)
                lows.append(low)
                if rows.stop == cut:
                    c_ref[pl.ds(2 * g + 2, 2)] = back(
                        slice(0, cut), jnp.concatenate(highs, axis=0), jnp.concatenate(lows, axis=0)
                    )
            else:
                late = slice(rows.start - cut, rows.stop - cut)
                v_refs[now][0, late, :] = high
                v_refs[now][1, late, :] = low

    rhs = point_rhs(0)
    for rows in steps:
        p_refs[0][rows, :] = dot(lhs_p_ref[rows, :], rhs)

    def several(j, carry):
        for i in range(unroll):
            phase(unroll * j + i, i % 2)
        return carry

    lax.fori_loop(0, pairs // unroll, several, 0)
    for g in range(pairs // unroll * unroll, pairs):
        phase(g, g % 2)
    finish(pairs - 1, v_refs[(pairs - 1) % 2])


def band_sum(recv_ref, rows):
    total = recv_ref[0, rows, :]
    for k in range(1, recv_ref.shape[0]):
        total = total + recv_ref[k, rows, :]
    return total


def row_pad(x, rows):
    return jnp.concatenate([x, jnp.zeros((rows - x.shape[0], x.shape[1]), jnp.float32)], axis=0)


def masked_density(total, live):
    rows = lax.broadcasted_iota(jnp.int32, total.shape, 0)
    density = jnp.where(live & (rows < 171), total, 0.0)
    return jnp.where((rows == 171) | (rows == 172), 1.0, density)


def energy_line(e_ref, part, weight_ref):
    return jnp.sum(e_ref[part] * weight_ref[...], axis=0, keepdims=True)


def forward(table, high, low):
    return dot(table, jnp.concatenate([high, high], axis=0)) + dot(table[:, :PROWS], low)


def start_blocks(recv_ref, lives, mt, b_ref, directions):
    lead = 48 * (len(lives) - 1)
    density = masked_density(row_pad(band_sum(recv_ref, slice(lead, recv_ref.shape[1])), PROWS), lives[0])
    if lead:
        total = band_sum(recv_ref, slice(0, lead))
        pieces = [total[:, 32 * i : 32 * i + 32] for i in range(4)]
        spread = jnp.concatenate([jnp.concatenate([p] * 4, axis=1) for p in pieces], axis=0)
        density = jnp.concatenate([density, masked_density(spread, lives[1])], axis=1)
    rows = directions * QROWS
    table = mt[...] if lead else mt[:rows, :]
    blocks = forward(table, *halves(density))
    b_ref[:directions] = blocks[:rows, :LANES].reshape(directions, QROWS, LANES)
    if lead:
        parts = blocks[:, LANES:].reshape(4, GROUP * QROWS, LANES)
        lane_group = lax.broadcasted_iota(jnp.int32, parts.shape[1:], 1) // 32
        chosen = parts[3]
        for i in range(3):
            chosen = jnp.where(lane_group == i, parts[i], chosen)
        b_ref[directions : directions + GROUP] = chosen.reshape(GROUP, QROWS, LANES)


def finish_blocks(c_ref, m_hl, lives, line, directions):
    rows = directions * QROWS
    sums = c_ref[2 : 2 + directions].reshape(rows, LANES)
    table = m_hl[:, :rows]
    if len(lives) > 1:
        table = m_hl[...]
        narrow = c_ref[directions + 2 : directions + 2 + GROUP].reshape(GROUP * QROWS, LANES)
        lane_group = lax.broadcasted_iota(jnp.int32, narrow.shape, 1) // 32
        spread = jnp.concatenate([jnp.where(lane_group == i, narrow, 0.0) for i in range(4)], axis=0)
        sums = jnp.concatenate([row_pad(sums, table.shape[1]), spread], axis=1)
    high, low = halves(sums)
    first = dot(table, high)
    ham = first[:PROWS] + first[PROWS:] + dot(table[:PROWS], low)
    wide = jnp.where(lives[0], ham[:171, :LANES], 0.0)
    if len(lives) == 1:
        return [wide]
    ham = ham[:, LANES:]
    kind = lax.broadcasted_iota(jnp.int32, (PROWS, LANES), 0)
    ham = jnp.where(kind == 171, line, ham)
    ham = sum(ham[:, 32 * i : 32 * i + 32] for i in range(4))
    packed = jnp.concatenate([ham[48 * i : 48 * i + 48] for i in range(4)], axis=1)
    return [jnp.where(lives[1], packed, 0.0), wide]


def chunk_kernel(base, narrow_base, copies, directions, owned_ref, recv_ref, *refs):
    mt, m_far, lhs_p, lhs_b, weight = refs[:5]
    out_ref, b_ref, c_ref, e_ref, p0, p1, v0, v1, m_hl, near_ref, sem = refs[5:]
    m_copy = pltpu.make_async_copy(m_far, m_hl, sem.at[copies])
    m_copy.start()
    lane = lax.broadcasted_iota(jnp.int32, (1, LANES), 1)
    lives = [base + lane < owned_ref[0:1, :]]
    pairs, part_of = directions // 2, lambda g: 0
    if narrow_base is not None:
        lives.append(narrow_base + lane % 32 < owned_ref[1:2, :])
        wide, filled = pairs, pairs + (directions - 3 * GROUP) // 2
        part_of = lambda g: jnp.where(g >= wide, 1, 0) + jnp.where(g >= filled, 1, 0)
        pairs = pairs + GROUP // 2
    e_ref[...] = jnp.zeros_like(e_ref)
    start_blocks(recv_ref, lives, mt, b_ref, directions)
    evaluate_blocks(pairs, 4 if narrow_base is None else 8, part_of, b_ref, c_ref, e_ref, lhs_p, lhs_b, (p0, p1), (v0, v1))
    energy = jnp.where(lives[0], energy_line(e_ref, 0, weight), 0.0)
    line = None
    if narrow_base is not None:
        line = energy_line(e_ref, 1, weight) + jnp.where(lane < 96, energy_line(e_ref, 2, weight), 0.0)
    m_copy.wait()
    target = near_ref if copies > 1 else out_ref.at[0]
    at = 0
    for piece in [jnp.broadcast_to(energy, (8, LANES))] + finish_blocks(c_ref, m_hl, lives, line, directions):
        target[at : at + piece.shape[0], :] = piece
        at += piece.shape[0]
    if copies > 1:
        leaving = [pltpu.make_async_copy(near_ref, out_ref.at[k], sem.at[k]) for k in range(copies)]
        for copy in leaving:
            copy.start()
        for copy in leaving:
            copy.wait()


def chunk_call(base, narrow_base, copies, directions, owned, recv, tables):
    narrow = narrow_base is not None
    tables = [tables[0], pltpu.with_memory_space_constraint(tables[1], pltpu.HBM)] + list(tables[2:])
    shape = (copies, 179 + 48 * narrow, LANES)
    blocks = directions + GROUP * narrow
    grid_rows = tables[2].shape[0]
    return pl.pallas_call(
        functools.partial(chunk_kernel, base, narrow_base, copies, directions),
        out_shape=(pltpu.VMEM if copies == 1 else pltpu.HBM)(shape, jnp.float32),
        in_specs=[pl.BlockSpec(memory_space=pltpu.VMEM)] * 3
        + [pl.BlockSpec(memory_space=pltpu.HBM)]
        + [pl.BlockSpec(memory_space=pltpu.VMEM)] * 3,
        out_specs=pl.BlockSpec(memory_space=pltpu.VMEM if copies == 1 else pltpu.HBM),
        scratch_shapes=[pltpu.VMEM((blocks + 2, QROWS, LANES), jnp.float32)] * 2
        + [pltpu.VMEM((1 + 2 * narrow, grid_rows, LANES), jnp.float32)]
        + [pltpu.VMEM((grid_rows, 2 * LANES), jnp.float32)] * 2
        + [pltpu.VMEM((2, grid_rows, 2 * LANES), jnp.bfloat16)] * 2
        + [pltpu.VMEM(tables[1].shape, jnp.bfloat16)]
        + [pltpu.VMEM(shape[1:], jnp.float32), pltpu.SemaphoreType.DMA((copies + 1,))],
        cost_estimate=pl.CostEstimate(flops=8_000_000_000, bytes_accessed=4_000_000, transcendentals=10_000_000),
        compiler_params=pltpu.CompilerParams(vmem_limit_bytes=18 * 1024 * 1024),
    )(owned, recv, *tables)


def table_kernel(gaunt_ref, waves_ref, y_ref, core_ref, rw_ref, mt_ref, m_far, lhs_p, lhs_b, weight_ref, *scratch):
    gt_ref, mf_ref, m_hl, sem = scratch
    entries, columns = gaunt_ref.shape
    pairs, grid = waves_ref.shape
    harmonics, directions = y_ref.shape
    gt_pad = jnp.concatenate([gaunt_ref[...], jnp.zeros((256 - entries, columns), jnp.float32)], axis=0)
    gt_pad = jnp.concatenate([gt_pad, jnp.zeros((256, 640 - columns), jnp.float32)], axis=1)
    turned = gt_pad.T
    gt_ref[0] = turned[:, :LANES]
    gt_ref[1] = turned[:, LANES:]
    mf_ref[...] = jnp.zeros_like(mf_ref)
    for q in range(pairs):
        for half in range(2):
            part = gt_ref[half, pl.ds(q, harmonics, stride=pairs), :]
            made = lax.dot_general(
                y_ref[...], part, (((0,), (0,)), ((), ())), precision=highest, preferred_element_type=jnp.float32
            )
            mf_ref[half, pl.ds(q, directions, stride=QROWS), :] = made
    m = jnp.concatenate([mf_ref[0], mf_ref[1]], axis=1)
    mh, ml = halves(m.T[:PROWS])
    m_hl[:PROWS, :] = mh
    m_hl[PROWS:, :] = ml
    m_copy = pltpu.make_async_copy(m_hl, m_far, sem.at[0])
    m_copy.start()
    m = m[:, :PROWS]
    row = lax.broadcasted_iota(jnp.int32, m.shape, 0)
    col = lax.broadcasted_iota(jnp.int32, m.shape, 1)
    kind = row % QROWS
    unit = (row < directions * QROWS) & (((kind == 21) & (col == 171)) | ((kind == 22) & (col == 172)))
    high, low = halves(jnp.where(unit, 1.0, m))
    mt_ref[...] = jnp.concatenate([high, low], axis=1)
    waves = waves_ref[...]
    back = lambda x: x.astype(jnp.float32)
    wh = back(waves.astype(jnp.bfloat16))
    wl = waves - wh
    core = core_ref[...]
    ch = back(core.astype(jnp.bfloat16))
    cm = back((core - ch).astype(jnp.bfloat16))
    cl = core - ch - cm
    gap = lambda n: jnp.zeros((n, grid), jnp.float32)
    stack = jnp.concatenate(
        [wh, ch, cl, gap(QROWS - pairs - 2), wh, gap(QROWS - pairs), wl, cm, gap(QROWS - pairs - 1), gap(32)], axis=0
    )
    stack = jnp.concatenate([stack, jnp.zeros((LANES, 512 - grid), jnp.float32)], axis=1)
    lhs_p[...] = stack.T[:grid, :96].astype(jnp.bfloat16)
    weight = -(4.0 * jnp.pi / directions) * rw_ref[...]
    bh, bl = halves(jnp.concatenate([waves * (SLOPE * weight), gap(QROWS - pairs)], axis=0))
    lhs_b[...] = jnp.concatenate([bh, bl], axis=0)
    wide = jnp.concatenate([jnp.broadcast_to(ENERGY * weight, (LANES, grid)), jnp.zeros((LANES, 512 - grid), jnp.float32)], axis=1)
    weight_ref[...] = wide.T[:grid]
    m_copy.wait()


def make_tables(gaunt, pair_waves, y_table, core, radial_weights):
    grid = core.shape[0]
    rows = 4 * GROUP * QROWS
    return pl.pallas_call(
        table_kernel,
        out_shape=(
            jax.ShapeDtypeStruct((rows, 2 * PROWS), jnp.bfloat16),
            pltpu.HBM((2 * PROWS, rows), jnp.bfloat16),
            jax.ShapeDtypeStruct((grid, 96), jnp.bfloat16),
            jax.ShapeDtypeStruct((2 * QROWS, grid), jnp.bfloat16),
            jax.ShapeDtypeStruct((grid, LANES), jnp.float32),
        ),
        in_specs=[pl.BlockSpec(memory_space=pltpu.VMEM)] * 5,
        out_specs=[pl.BlockSpec(memory_space=pltpu.VMEM), pl.BlockSpec(memory_space=pltpu.HBM)]
        + [pl.BlockSpec(memory_space=pltpu.VMEM)] * 3,
        scratch_shapes=[
            pltpu.VMEM((2, 640, LANES), jnp.float32),
            pltpu.VMEM((2, rows, LANES), jnp.float32),
            pltpu.VMEM((2 * PROWS, rows), jnp.bfloat16),
            pltpu.SemaphoreType.DMA((1,)),
        ],
        cost_estimate=pl.CostEstimate(flops=2_000_000_000, bytes_accessed=4_000_000, transcendentals=0),
        compiler_params=pltpu.CompilerParams(vmem_limit_bytes=18 * 1024 * 1024),
    )(gaunt, pair_waves, y_table, core.reshape(1, grid), radial_weights.reshape(1, grid))


def send_kernel(first, narrow, block_ref, out_ref, near_ref, *scratch):
    entries = block_ref.shape[0]
    tail_ref, pack_ref, sem = scratch if narrow is not None else (None, None, *scratch)
    lead = 48 if narrow is not None else 0
    arrivals = [
        pltpu.make_async_copy(block_ref.at[:, 0, pl.ds(first + LANES * k, LANES)], near_ref.at[k], sem.at[k])
        for k in range(8)
    ]
    if narrow is not None:
        tail = pltpu.make_async_copy(block_ref.at[:, 0, pl.ds(narrow, 256)], tail_ref, sem.at[16])
        tail.start()
    for copy in arrivals:
        copy.start()
    leaving = []
    if narrow is not None:
        tail.wait()
        rows = row_pad(tail_ref[...], PROWS)
        for k in range(8):
            own = rows[:, 32 * k : 32 * k + 32]
            pack_ref[k] = jnp.concatenate([own[48 * i : 48 * i + 48] for i in range(4)], axis=1)
        leaving.append(pltpu.make_async_copy(pack_ref, out_ref.at[:, pl.ds(0, 48)], sem.at[17]))
        leaving[0].start()
    for k in range(8):
        arrivals[k].wait()
        copy = pltpu.make_async_copy(near_ref.at[k], out_ref.at[k, pl.ds(lead, entries)], sem.at[8 + k])
        copy.start()
        leaving.append(copy)
    for copy in leaving:
        copy.wait()


def send_call(first, narrow, rows):
    entries = rows.shape[0]
    scratch = [pltpu.VMEM((8, entries, LANES), jnp.float32)]
    if narrow is not None:
        scratch += [pltpu.VMEM((entries, 256), jnp.float32), pltpu.VMEM((8, 48, LANES), jnp.float32)]
    return pl.pallas_call(
        functools.partial(send_kernel, first, narrow),
        out_shape=pltpu.HBM((8, entries + (48 if narrow is not None else 0), LANES), jnp.float32),
        in_specs=[pl.BlockSpec(memory_space=pltpu.HBM)],
        out_specs=pl.BlockSpec(memory_space=pltpu.HBM),
        scratch_shapes=scratch + [pltpu.SemaphoreType.DMA((18,))],
        cost_estimate=pl.CostEstimate(flops=100_000_000, bytes_accessed=1_500_000, transcendentals=0),
        compiler_params=pltpu.CompilerParams(vmem_limit_bytes=6 * 1024 * 1024),
    )(rows)


def assemble_kernel(a_ref, b_ref, ham_ref, energy_far, tail_ref, energy_ref, sem):
    copies = []
    for k in range(8):
        for part, ref, at in ((0, a_ref, 56), (1, b_ref, 8)):
            target = ham_ref.at[:, pl.ds(1024 * part + LANES * k, LANES)]
            copies.append(pltpu.make_async_copy(ref.at[k, pl.ds(at, 171)], target, sem.at[8 * part + k]))
    for copy in copies:
        copy.start()
    for i in range(4):
        rows = jnp.concatenate([a_ref[k, 8:56, 32 * i : 32 * i + 32] for k in range(8)], axis=1)
        if i < 3:
            tail_ref[48 * i : 48 * i + 48, :] = rows
        else:
            tail_ref[144:171, :] = rows[:27]
            energy_ref[16:18, :] = jnp.concatenate([rows[27:28, :LANES], rows[27:28, LANES:]], axis=0)
    tail = pltpu.make_async_copy(tail_ref, ham_ref.at[:, pl.ds(2048, 256)], sem.at[16])
    tail.start()
    for k in range(8):
        energy_ref[k : k + 1, :] = a_ref[k, 0:1, :]
        energy_ref[8 + k : 9 + k, :] = b_ref[k, 0:1, :]
    energies = pltpu.make_async_copy(energy_ref, energy_far, sem.at[17])
    energies.start()
    for copy in copies:
        copy.wait()
    tail.wait()
    energies.wait()


def assemble(all_a, all_b):
    return pl.pallas_call(
        assemble_kernel,
        out_shape=(pltpu.HBM((171, 2304), jnp.float32), pltpu.HBM((18, LANES), jnp.float32)),
        in_specs=[pl.BlockSpec(memory_space=pltpu.VMEM)] * 2,
        out_specs=[pl.BlockSpec(memory_space=pltpu.HBM)] * 2,
        scratch_shapes=[
            pltpu.VMEM((171, 256), jnp.float32),
            pltpu.VMEM((18, LANES), jnp.float32),
            pltpu.SemaphoreType.DMA((18,)),
        ],
        cost_estimate=pl.CostEstimate(flops=100_000_000, bytes_accessed=3_000_000, transcendentals=0),
        compiler_params=pltpu.CompilerParams(vmem_limit_bytes=8 * 1024 * 1024),
    )(all_a, all_b)


def per_device(dens_part, counts, gaunt, pair_waves, y_table, core, radial_weights):
    band_index = lax.axis_index("band").astype(jnp.int32)
    widths = jnp.where(lax.broadcasted_iota(jnp.int32, (2, LANES), 0) == 0, LANES, 32)
    owned = counts[0].astype(jnp.int32) - band_index * widths
    directions = y_table.shape[1]
    rows = pltpu.with_memory_space_constraint(dens_part.transpose(1, 0, 2), pltpu.HBM)
    send_a = send_call(0, 2048, rows)
    recv_a = lax.all_to_all(send_a, "band", 0, 0, tiled=True)
    send_b = send_call(1024, None, rows)
    recv_b = lax.all_to_all(send_b, "band", 0, 0, tiled=True)
    tables = make_tables(gaunt, pair_waves, y_table, core, radial_weights)
    out_a = chunk_call(0, 2048, 8, directions, owned, recv_a, tables)
    all_a = lax.all_to_all(out_a, "band", 0, 0, tiled=True)
    out_b = chunk_call(1024, None, 1, directions, owned, recv_b, tables)
    all_b = lax.all_gather(out_b[0], "band", axis=0)
    ham, energy = assemble(all_a, all_b)
    return ham, energy.reshape(18 * LANES)


def solution(mesh):
    return jax.shard_map(
        per_device,
        mesh=mesh,
        in_specs=(P("band", None, "domain"), P("domain"), P(), P(), P(), P(), P()),
        out_specs=(P(None, "domain"), P("domain")),
        check_vma=False,
    )
```

```python
import functools

import jax
import jax.numpy as jnp
from jax import lax
from jax.experimental import pallas as pl
from jax.experimental.pallas import tpu as pltpu
from jax.sharding import PartitionSpec as P

highest = lax.Precision.HIGHEST
LANES = 128
QROWS = 32
PROWS = 192
GROUP = 14
RADIUS = 0.6203504908994
SLOPE = 0.44 * RADIUS / 3.0 / 7.8**2
SLOPE_SHIFT = 0.5 * (0.44 / 7.8) / SLOPE
SLOPE_REST = 0.9847450218426965 / SLOPE - SLOPE_SHIFT**2
ENERGY = 0.44 / 7.8
ENERGY_SHIFT = 0.7385587663820224 / ENERGY


def halves(x):
    high = x.astype(jnp.bfloat16)
    return high, (x - high.astype(jnp.float32)).astype(jnp.bfloat16)


def dot(a, b):
    return jnp.dot(a, b, preferred_element_type=jnp.float32)


def point_terms(points):
    log = jnp.log2(points * points + 0.25)
    t = jnp.exp2(log * (1.0 / 6.0))
    square = t * t
    share = 1.0 / (t + RADIUS / 7.8)
    energy = (square * square) * (share + ENERGY_SHIFT)
    shifted = share + SLOPE_SHIFT
    return energy, (points * (1.0 / square)) * (shifted * shifted + SLOPE_REST)


def evaluate_blocks(pairs, unroll, part_of, b_ref, c_ref, e_ref, lhs_p_ref, lhs_b_ref, p_refs, v_refs):
    grid_rows = lhs_p_ref.shape[0]
    cut = 208
    steps = [slice(0, 64), slice(64, 128), slice(128, 208), slice(208, 272), slice(272, 336), slice(336, 400)]

    def point_rhs(g):
        pieces = b_ref[pl.ds(2 * g, 2)]
        high, low = halves(jnp.concatenate([pieces[0], pieces[1]], axis=1))
        return jnp.concatenate([high, low, high], axis=0)

    def back(cols, high, low):
        first = dot(lhs_b_ref[:, cols], high)
        total = first[:QROWS] + first[QROWS:] + dot(lhs_b_ref[:QROWS, cols], low)
        return jnp.stack([total[:, :LANES], total[:, LANES:]])

    def finish(g, v_ref):
        c_ref[pl.ds(2 * g + 2, 2)] += back(slice(cut, grid_rows), v_ref[0, : grid_rows - cut, :], v_ref[1, : grid_rows - cut, :])

    def phase(g, now):
        other = 1 - now
        part = part_of(g)
        rhs = point_rhs(g + 1)
        finish(g - 1, v_refs[other])
        highs, lows = [], []
        for rows in steps:
            p_refs[other][rows, :] = dot(lhs_p_ref[rows, :], rhs)
            energy, potential = point_terms(p_refs[now][rows, :])
            e_ref[part, rows, :] += energy[:, :LANES] + energy[:, LANES:]
            high, low = halves(potential)
            if rows.stop <= cut:
                highs.append(high)
                lows.append(low)
                if rows.stop == cut:
                    c_ref[pl.ds(2 * g + 2, 2)] = back(
                        slice(0, cut), jnp.concatenate(highs, axis=0), jnp.concatenate(lows, axis=0)
                    )
            else:
                late = slice(rows.start - cut, rows.stop - cut)
                v_refs[now][0, late, :] = high
                v_refs[now][1, late, :] = low

    rhs = point_rhs(0)
    for rows in steps:
        p_refs[0][rows, :] = dot(lhs_p_ref[rows, :], rhs)

    def several(j, carry):
        for i in range(unroll):
            phase(unroll * j + i, i % 2)
        return carry

    lax.fori_loop(0, pairs // unroll, several, 0)
    for g in range(pairs // unroll * unroll, pairs):
        phase(g, g % 2)
    finish(pairs - 1, v_refs[(pairs - 1) % 2])


def band_sum(recv_ref, rows):
    total = recv_ref[0, rows, :]
    for k in range(1, recv_ref.shape[0]):
        total = total + recv_ref[k, rows, :]
    return total


def row_pad(x, rows):
    return jnp.concatenate([x, jnp.zeros((rows - x.shape[0], x.shape[1]), jnp.float32)], axis=0)


def masked_density(total, live):
    rows = lax.broadcasted_iota(jnp.int32, total.shape, 0)
    density = jnp.where(live & (rows < 171), total, 0.0)
    return jnp.where((rows == 171) | (rows == 172), 1.0, density)


def energy_line(e_ref, part, weight_ref):
    return jnp.sum(e_ref[part] * weight_ref[...], axis=0, keepdims=True)


def forward(table, high, low):
    return dot(table, jnp.concatenate([high, high], axis=0)) + dot(table[:, :PROWS], low)


def start_blocks(recv_ref, lives, mt, b_ref, directions):
    lead = 48 * (len(lives) - 1)
    density = masked_density(row_pad(band_sum(recv_ref, slice(lead, recv_ref.shape[1])), PROWS), lives[0])
    if lead:
        total = band_sum(recv_ref, slice(0, lead))
        pieces = [total[:, 32 * i : 32 * i + 32] for i in range(4)]
        spread = jnp.concatenate([jnp.concatenate([p] * 4, axis=1) for p in pieces], axis=0)
        density = jnp.concatenate([density, masked_density(spread, lives[1])], axis=1)
    rows = directions * QROWS
    table = mt[...] if lead else mt[:rows, :]
    blocks = forward(table, *halves(density))
    b_ref[:directions] = blocks[:rows, :LANES].reshape(directions, QROWS, LANES)
    if lead:
        parts = blocks[:, LANES:].reshape(4, GROUP * QROWS, LANES)
        lane_group = lax.broadcasted_iota(jnp.int32, parts.shape[1:], 1) // 32
        chosen = parts[3]
        for i in range(3):
            chosen = jnp.where(lane_group == i, parts[i], chosen)
        b_ref[directions : directions + GROUP] = chosen.reshape(GROUP, QROWS, LANES)


def finish_blocks(c_ref, m_hl, lives, line, directions):
    rows = directions * QROWS
    sums = c_ref[2 : 2 + directions].reshape(rows, LANES)
    table = m_hl[:, :rows]
    if len(lives) > 1:
        table = m_hl[...]
        narrow = c_ref[directions + 2 : directions + 2 + GROUP].reshape(GROUP * QROWS, LANES)
        lane_group = lax.broadcasted_iota(jnp.int32, narrow.shape, 1) // 32
        spread = jnp.concatenate([jnp.where(lane_group == i, narrow, 0.0) for i in range(4)], axis=0)
        sums = jnp.concatenate([row_pad(sums, table.shape[1]), spread], axis=1)
    high, low = halves(sums)
    first = dot(table, high)
    ham = first[:PROWS] + first[PROWS:] + dot(table[:PROWS], low)
    wide = jnp.where(lives[0], ham[:171, :LANES], 0.0)
    if len(lives) == 1:
        return [wide]
    ham = ham[:, LANES:]
    kind = lax.broadcasted_iota(jnp.int32, (PROWS, LANES), 0)
    ham = jnp.where(kind == 171, line, ham)
    ham = sum(ham[:, 32 * i : 32 * i + 32] for i in range(4))
    packed = jnp.concatenate([ham[48 * i : 48 * i + 48] for i in range(4)], axis=1)
    return [jnp.where(lives[1], packed, 0.0), wide]


def chunk_kernel(base, narrow_base, copies, directions, owned_ref, recv_ref, *refs):
    mt, m_far, lhs_p, lhs_b, weight = refs[:5]
    out_ref, b_ref, c_ref, e_ref, p0, p1, v0, v1, m_hl, near_ref, sem = refs[5:]
    m_copy = pltpu.make_async_copy(m_far, m_hl, sem.at[copies])
    m_copy.start()
    lane = lax.broadcasted_iota(jnp.int32, (1, LANES), 1)
    lives = [base + lane < owned_ref[0:1, :]]
    pairs, part_of = directions // 2, lambda g: 0
    if narrow_base is not None:
        lives.append(narrow_base + lane % 32 < owned_ref[1:2, :])
        wide, filled = pairs, pairs + (directions - 3 * GROUP) // 2
        part_of = lambda g: jnp.where(g >= wide, 1, 0) + jnp.where(g >= filled, 1, 0)
        pairs = pairs + GROUP // 2
    e_ref[...] = jnp.zeros_like(e_ref)
    start_blocks(recv_ref, lives, mt, b_ref, directions)
    evaluate_blocks(pairs, 12 if narrow_base is None else 16, part_of, b_ref, c_ref, e_ref, lhs_p, lhs_b, (p0, p1), (v0, v1))
    energy = jnp.where(lives[0], energy_line(e_ref, 0, weight), 0.0)
    line = None
    if narrow_base is not None:
        line = energy_line(e_ref, 1, weight) + jnp.where(lane < 96, energy_line(e_ref, 2, weight), 0.0)
    m_copy.wait()
    target = near_ref if copies > 1 else out_ref.at[0]
    at = 0
    for piece in [jnp.broadcast_to(energy, (8, LANES))] + finish_blocks(c_ref, m_hl, lives, line, directions):
        target[at : at + piece.shape[0], :] = piece
        at += piece.shape[0]
    if copies > 1:
        leaving = [pltpu.make_async_copy(near_ref, out_ref.at[k], sem.at[k]) for k in range(copies)]
        for copy in leaving:
            copy.start()
        for copy in leaving:
            copy.wait()


def chunk_call(base, narrow_base, copies, directions, owned, recv, tables):
    narrow = narrow_base is not None
    tables = [tables[0], pltpu.with_memory_space_constraint(tables[1], pltpu.HBM)] + list(tables[2:])
    shape = (copies, 179 + 48 * narrow, LANES)
    blocks = directions + GROUP * narrow
    grid_rows = tables[2].shape[0]
    return pl.pallas_call(
        functools.partial(chunk_kernel, base, narrow_base, copies, directions),
        out_shape=(pltpu.VMEM if copies == 1 else pltpu.HBM)(shape, jnp.float32),
        in_specs=[pl.BlockSpec(memory_space=pltpu.VMEM)] * 3
        + [pl.BlockSpec(memory_space=pltpu.HBM)]
        + [pl.BlockSpec(memory_space=pltpu.VMEM)] * 3,
        out_specs=pl.BlockSpec(memory_space=pltpu.VMEM if copies == 1 else pltpu.HBM),
        scratch_shapes=[pltpu.VMEM((blocks + 2, QROWS, LANES), jnp.float32)] * 2
        + [pltpu.VMEM((1 + 2 * narrow, grid_rows, LANES), jnp.float32)]
        + [pltpu.VMEM((grid_rows, 2 * LANES), jnp.float32)] * 2
        + [pltpu.VMEM((2, grid_rows, 2 * LANES), jnp.bfloat16)] * 2
        + [pltpu.VMEM(tables[1].shape, jnp.bfloat16)]
        + [pltpu.VMEM(shape[1:], jnp.float32), pltpu.SemaphoreType.DMA((copies + 1,))],
        cost_estimate=pl.CostEstimate(flops=8_000_000_000, bytes_accessed=4_000_000, transcendentals=10_000_000),
        compiler_params=pltpu.CompilerParams(vmem_limit_bytes=18 * 1024 * 1024),
    )(owned, recv, *tables)


def table_kernel(gaunt_ref, waves_ref, y_ref, core_ref, rw_ref, mt_ref, m_far, lhs_p, lhs_b, weight_ref, *scratch):
    gt_ref, mf_ref, m_hl, sem = scratch
    entries, columns = gaunt_ref.shape
    pairs, grid = waves_ref.shape
    harmonics, directions = y_ref.shape
    gt_pad = jnp.concatenate([gaunt_ref[...], jnp.zeros((256 - entries, columns), jnp.float32)], axis=0)
    gt_pad = jnp.concatenate([gt_pad, jnp.zeros((256, 640 - columns), jnp.float32)], axis=1)
    turned = gt_pad.T
    gt_ref[0] = turned[:, :LANES]
    gt_ref[1] = turned[:, LANES:]
    mf_ref[...] = jnp.zeros_like(mf_ref)
    for q in range(pairs):
        for half in range(2):
            part = gt_ref[half, pl.ds(q, harmonics, stride=pairs), :]
            made = lax.dot_general(
                y_ref[...], part, (((0,), (0,)), ((), ())), precision=highest, preferred_element_type=jnp.float32
            )
            mf_ref[half, pl.ds(q, directions, stride=QROWS), :] = made
    m = jnp.concatenate([mf_ref[0], mf_ref[1]], axis=1)
    mh, ml = halves(m.T[:PROWS])
    m_hl[:PROWS, :] = mh
    m_hl[PROWS:, :] = ml
    m_copy = pltpu.make_async_copy(m_hl, m_far, sem.at[0])
    m_copy.start()
    m = m[:, :PROWS]
    row = lax.broadcasted_iota(jnp.int32, m.shape, 0)
    col = lax.broadcasted_iota(jnp.int32, m.shape, 1)
    kind = row % QROWS
    unit = (row < directions * QROWS) & (((kind == 21) & (col == 171)) | ((kind == 22) & (col == 172)))
    high, low = halves(jnp.where(unit, 1.0, m))
    mt_ref[...] = jnp.concatenate([high, low], axis=1)
    waves = waves_ref[...]
    back = lambda x: x.astype(jnp.float32)
    wh = back(waves.astype(jnp.bfloat16))
    wl = waves - wh
    core = core_ref[...]
    ch = back(core.astype(jnp.bfloat16))
    cm = back((core - ch).astype(jnp.bfloat16))
    cl = core - ch - cm
    gap = lambda n: jnp.zeros((n, grid), jnp.float32)
    stack = jnp.concatenate(
        [wh, ch, cl, gap(QROWS - pairs - 2), wh, gap(QROWS - pairs), wl, cm, gap(QROWS - pairs - 1), gap(32)], axis=0
    )
    stack = jnp.concatenate([stack, jnp.zeros((LANES, 512 - grid), jnp.float32)], axis=1)
    lhs_p[...] = stack.T[:grid, :96].astype(jnp.bfloat16)
    weight = -(4.0 * jnp.pi / directions) * rw_ref[...]
    bh, bl = halves(jnp.concatenate([waves * (SLOPE * weight), gap(QROWS - pairs)], axis=0))
    lhs_b[...] = jnp.concatenate([bh, bl], axis=0)
    wide = jnp.concatenate([jnp.broadcast_to(ENERGY * weight, (LANES, grid)), jnp.zeros((LANES, 512 - grid), jnp.float32)], axis=1)
    weight_ref[...] = wide.T[:grid]
    m_copy.wait()


def make_tables(gaunt, pair_waves, y_table, core, radial_weights):
    grid = core.shape[0]
    rows = 4 * GROUP * QROWS
    return pl.pallas_call(
        table_kernel,
        out_shape=(
            jax.ShapeDtypeStruct((rows, 2 * PROWS), jnp.bfloat16),
            pltpu.HBM((2 * PROWS, rows), jnp.bfloat16),
            jax.ShapeDtypeStruct((grid, 96), jnp.bfloat16),
            jax.ShapeDtypeStruct((2 * QROWS, grid), jnp.bfloat16),
            jax.ShapeDtypeStruct((grid, LANES), jnp.float32),
        ),
        in_specs=[pl.BlockSpec(memory_space=pltpu.VMEM)] * 5,
        out_specs=[pl.BlockSpec(memory_space=pltpu.VMEM), pl.BlockSpec(memory_space=pltpu.HBM)]
        + [pl.BlockSpec(memory_space=pltpu.VMEM)] * 3,
        scratch_shapes=[
            pltpu.VMEM((2, 640, LANES), jnp.float32),
            pltpu.VMEM((2, rows, LANES), jnp.float32),
            pltpu.VMEM((2 * PROWS, rows), jnp.bfloat16),
            pltpu.SemaphoreType.DMA((1,)),
        ],
        cost_estimate=pl.CostEstimate(flops=2_000_000_000, bytes_accessed=4_000_000, transcendentals=0),
        compiler_params=pltpu.CompilerParams(vmem_limit_bytes=18 * 1024 * 1024),
    )(gaunt, pair_waves, y_table, core.reshape(1, grid), radial_weights.reshape(1, grid))


def send_kernel(first, narrow, block_ref, out_ref, near_ref, *scratch):
    entries = block_ref.shape[0]
    tail_ref, pack_ref, sem = scratch if narrow is not None else (None, None, *scratch)
    lead = 48 if narrow is not None else 0
    arrivals = [
        pltpu.make_async_copy(block_ref.at[:, 0, pl.ds(first + LANES * k, LANES)], near_ref.at[k], sem.at[k])
        for k in range(8)
    ]
    if narrow is not None:
        tail = pltpu.make_async_copy(block_ref.at[:, 0, pl.ds(narrow, 256)], tail_ref, sem.at[16])
        tail.start()
    for copy in arrivals:
        copy.start()
    leaving = []
    if narrow is not None:
        tail.wait()
        rows = row_pad(tail_ref[...], PROWS)
        for k in range(8):
            own = rows[:, 32 * k : 32 * k + 32]
            pack_ref[k] = jnp.concatenate([own[48 * i : 48 * i + 48] for i in range(4)], axis=1)
        leaving.append(pltpu.make_async_copy(pack_ref, out_ref.at[:, pl.ds(0, 48)], sem.at[17]))
        leaving[0].start()
    for k in range(8):
        arrivals[k].wait()
        copy = pltpu.make_async_copy(near_ref.at[k], out_ref.at[k, pl.ds(lead, entries)], sem.at[8 + k])
        copy.start()
        leaving.append(copy)
    for copy in leaving:
        copy.wait()


def send_call(first, narrow, rows):
    entries = rows.shape[0]
    scratch = [pltpu.VMEM((8, entries, LANES), jnp.float32)]
    if narrow is not None:
        scratch += [pltpu.VMEM((entries, 256), jnp.float32), pltpu.VMEM((8, 48, LANES), jnp.float32)]
    return pl.pallas_call(
        functools.partial(send_kernel, first, narrow),
        out_shape=pltpu.HBM((8, entries + (48 if narrow is not None else 0), LANES), jnp.float32),
        in_specs=[pl.BlockSpec(memory_space=pltpu.HBM)],
        out_specs=pl.BlockSpec(memory_space=pltpu.HBM),
        scratch_shapes=scratch + [pltpu.SemaphoreType.DMA((18,))],
        cost_estimate=pl.CostEstimate(flops=100_000_000, bytes_accessed=1_500_000, transcendentals=0),
        compiler_params=pltpu.CompilerParams(vmem_limit_bytes=6 * 1024 * 1024),
    )(rows)


def assemble_kernel(a_ref, b_ref, ham_ref, energy_far, tail_ref, energy_ref, sem):
    copies = []
    for k in range(8):
        for part, ref, at in ((0, a_ref, 56), (1, b_ref, 8)):
            target = ham_ref.at[:, pl.ds(1024 * part + LANES * k, LANES)]
            copies.append(pltpu.make_async_copy(ref.at[k, pl.ds(at, 171)], target, sem.at[8 * part + k]))
    for copy in copies:
        copy.start()
    for i in range(4):
        rows = jnp.concatenate([a_ref[k, 8:56, 32 * i : 32 * i + 32] for k in range(8)], axis=1)
        if i < 3:
            tail_ref[48 * i : 48 * i + 48, :] = rows
        else:
            tail_ref[144:171, :] = rows[:27]
            energy_ref[16:18, :] = jnp.concatenate([rows[27:28, :LANES], rows[27:28, LANES:]], axis=0)
    tail = pltpu.make_async_copy(tail_ref, ham_ref.at[:, pl.ds(2048, 256)], sem.at[16])
    tail.start()
    for k in range(8):
        energy_ref[k : k + 1, :] = a_ref[k, 0:1, :]
        energy_ref[8 + k : 9 + k, :] = b_ref[k, 0:1, :]
    energies = pltpu.make_async_copy(energy_ref, energy_far, sem.at[17])
    energies.start()
    for copy in copies:
        copy.wait()
    tail.wait()
    energies.wait()


def assemble(all_a, all_b):
    return pl.pallas_call(
        assemble_kernel,
        out_shape=(pltpu.HBM((171, 2304), jnp.float32), pltpu.HBM((18, LANES), jnp.float32)),
        in_specs=[pl.BlockSpec(memory_space=pltpu.VMEM)] * 2,
        out_specs=[pl.BlockSpec(memory_space=pltpu.HBM)] * 2,
        scratch_shapes=[
            pltpu.VMEM((171, 256), jnp.float32),
            pltpu.VMEM((18, LANES), jnp.float32),
            pltpu.SemaphoreType.DMA((18,)),
        ],
        cost_estimate=pl.CostEstimate(flops=100_000_000, bytes_accessed=3_000_000, transcendentals=0),
        compiler_params=pltpu.CompilerParams(vmem_limit_bytes=8 * 1024 * 1024),
    )(all_a, all_b)


def per_device(dens_part, counts, gaunt, pair_waves, y_table, core, radial_weights):
    band_index = lax.axis_index("band").astype(jnp.int32)
    widths = jnp.where(lax.broadcasted_iota(jnp.int32, (2, LANES), 0) == 0, LANES, 32)
    owned = counts[0].astype(jnp.int32) - band_index * widths
    directions = y_table.shape[1]
    rows = pltpu.with_memory_space_constraint(dens_part.transpose(1, 0, 2), pltpu.HBM)
    send_a = send_call(0, 2048, rows)
    recv_a = lax.all_to_all(send_a, "band", 0, 0, tiled=True)
    send_b = send_call(1024, None, rows)
    recv_b = lax.all_to_all(send_b, "band", 0, 0, tiled=True)
    tables = make_tables(gaunt, pair_waves, y_table, core, radial_weights)
    out_a = chunk_call(0, 2048, 8, directions, owned, recv_a, tables)
    all_a = lax.all_to_all(out_a, "band", 0, 0, tiled=True)
    out_b = chunk_call(1024, None, 1, directions, owned, recv_b, tables)
    all_b = lax.all_gather(out_b[0], "band", axis=0)
    ham, energy = assemble(all_a, all_b)
    return ham, energy.reshape(18 * LANES)


def solution(mesh):
    return jax.shard_map(
        per_device,
        mesh=mesh,
        in_specs=(P("band", None, "domain"), P("domain"), P(), P(), P(), P(), P()),
        out_specs=(P(None, "domain"), P("domain")),
        check_vma=False,
    )
```
